32 devices in a mesh: net: 4 (over y, x), line: 8 (over z, core).
Axes of the slice: x: 2, y: 2, z: 4, core: 2. Of those that a mesh axis runs over, the one named last changes fastest.
Arguments:
- conductance_inverse: float32 [4, 4096, 4096], P('net', 'line'), may hold values from -0.5 to 4.5, as said below
- prior_voltage: float32 [4, 96, 4096], P('net', None, 'line'), may hold values from -6 to 6
- sources: float32 [3, 4, 4096], P(None, 'net', 'line'), may hold values from -6 to 6
- fault_node: int32 [96], replicated, may hold values from 0 to 16383
- fault_conductance: float32 [96], replicated, may hold values from 0.5 to 4
- terminal_node: int32 [4, 3, 4096], P('net', None, 'line'), may hold values from 0 to 4095
- ownership: int32 [4, 4096], P('net', 'line'), may hold values from 0 to 1, as said below
- partner: int32 [4, 4096], P('net', 'line'), may hold values from 0 to 31, as said below
- delay_steps: int32 [4, 4096], P('net', 'line'), may hold values from 1 to 4, as said below
- surge_conductance: float32 [4, 4096], P('net', 'line'), may hold values from 0.2 to 1
- pole_wave: float32 [4, 6, 4096], P('net', None, 'line'), may hold values from 0.2 to 0.95
- residue_wave: float32 [4, 6, 3, 3, 4096], P('net', None, None, None, 'line'), may hold values from -1 to 1
- pole_admit: float32 [4, 6, 4096], P('net', None, 'line'), may hold values from 0.2 to 0.95
- residue_admit: float32 [4, 6, 3, 3, 4096], P('net', None, None, None, 'line'), may hold values from -1 to 1
- wave_state: float32 [4, 6, 3, 96, 4096], P('net', None, None, None, 'line'), may hold values from -4 to 4
- admit_state: float32 [4, 6, 3, 96, 4096], P('net', None, None, None, 'line'), may hold values from -4 to 4
- wave_history: float32 [4, 4, 3, 96, 4096], P('net', None, None, None, 'line'), may hold values from -6 to 6
Outputs:
- final_voltage: float32 [4, 96, 4096], P('net', None, 'line')
- end_current: float32 [4, 3, 96, 4096], P('net', None, None, 'line')
The draws below stay inside these ranges and needn't reach their ends.
Inputs may be any that keep to these rules, and one draw needn't show every extreme that they name: `conductance_inverse`: each block is exactly symmetric. `ownership`: A slot is live exactly when the slot of the same number j % 512 at its partner owner is live; the number of live slots differs from owner to owner. The far end of slot j lies in the slot of the same number j % 512 at the partner owner, the partner of that slot is the first owner again, never the owner itself, and at most 17 live slots of one owner have the same partner; this many occur. `delay_steps`: equal at both ends of a line.
All inputs are finite; a program needn't handle non-finite values.
Results may differ from the reference program's by a relative error of at most 0.0003.
Values sent between devices are 32-bit elements; how exact they have to be, the bound alone decides.
A program may use at most 128 MiB of HBM per device.

```python
import math
from functools import partial
import jax
import jax.numpy as jnp
from jax import lax

NODES = 4096
SCENARIOS = 96
POLES = 6
STEPS = 3
DELAY_MAX = 4
SLOTS = 512
SUBS = 4
LINE_SLOTS = 4096
N_LINE = 8


def pair_tables(key):
    devices = SUBS * (LINE_SLOTS // SLOTS)
    anchor = jax.random.randint(jax.random.fold_in(key, 101), (), 0, devices)
    others = jax.random.permutation(jax.random.fold_in(key, 102), devices - 2) + 2
    flip_table = jnp.concatenate([jnp.ones((1,), jnp.int32), others.astype(jnp.int32)])
    slot_range = jnp.arange(SLOTS, dtype=jnp.int32)
    flip_mask = flip_table[slot_range % (devices - 1)]
    device_range = jnp.arange(devices, dtype=jnp.int32)
    partners = jnp.bitwise_xor(device_range[:, None], flip_mask[None, :])
    relabel = jnp.bitwise_xor(device_range, anchor)
    lowest = SLOTS // 6
    counts = jnp.where(relabel < 2, SLOTS, lowest + (relabel - 2) * (SLOTS - lowest) // (devices - 2))
    is_live = (slot_range[None, :] < counts[:, None]) & (slot_range[None, :] < counts[partners])
    return (partners, is_live, device_range, slot_range)


def draw_ownership(key, part):
    partners, is_live, device_range, slot_range = pair_tables(key)
    return is_live.astype(jnp.int32).reshape(SUBS, LINE_SLOTS)


def draw_partner(key, part):
    partners, is_live, device_range, slot_range = pair_tables(key)
    return partners.astype(jnp.int32).reshape(SUBS, LINE_SLOTS)


def draw_delay_steps(key, part):
    partners, is_live, device_range, slot_range = pair_tables(key)
    table = jax.random.randint(jax.random.fold_in(key, 103), partners.shape, 1, DELAY_MAX + 1)
    lower = jnp.minimum(device_range[:, None], partners)
    delays = table[lower, slot_range[None, :]]
    return delays.astype(jnp.int32).reshape(SUBS, LINE_SLOTS)


def draw_conductance_inverse(key, part):

    def one_block(index):
        block_key = jax.random.fold_in(key, index + 7)
        raw = jax.random.normal(jax.random.fold_in(block_key, 1), (NODES, NODES), jnp.float32)
        spread = (raw + raw.T) * (0.008 / math.sqrt(2.0))
        diagonal = jnp.exp(jax.random.uniform(jax.random.fold_in(block_key, 2), (NODES,), jnp.float32, math.log(1.5), math.log(4.0)))
        return spread + jnp.diag(diagonal)
    return lax.map(one_block, jnp.arange(SUBS, dtype=jnp.int32)).astype(jnp.float32)


def touch_ends(result, rng, smallest, high):
    longest = result.shape.index(max(result.shape))
    spots = []
    for shift in (0, 1):
        where = [jax.random.randint(jax.random.fold_in(rng, axis), (), 0, length) for axis, length in enumerate(result.shape)]
        where[longest] = (where[longest] + shift) % result.shape[longest]
        spots.append(tuple(where))
    return result.at[spots[0]].set(smallest).at[spots[1]].set(high)


def levels(own_key, extent, pieces, smallest, high):
    def one(axis_at, parts):
        draws = jax.random.uniform(jax.random.fold_in(jax.random.fold_in(own_key, 6), axis_at), (parts,), jnp.float32, smallest / len(pieces), high / len(pieces))
        return jnp.repeat(jnp.exp(draws), extent[axis_at] // parts).reshape((-1,) + (1,) * (len(extent) - axis_at - 1))

    loudness = one(*pieces[0])
    for cut in pieces[1:]:
        loudness = loudness * one(*cut)
    return loudness


def noise(own_key, dims, scale, bound, cuts=(), kind=jnp.bfloat16):
    loudness = levels(own_key, dims, cuts, -0.22, 0.18) if cuts else 1.0
    result = jax.random.normal(own_key, dims, jnp.float32) * scale * loudness
    return jnp.minimum(jnp.maximum(result, -bound), bound).astype(kind)


def setup_inputs(seed: int = 0) -> dict:
    splits = jax.random.split(jax.random.key(seed), 18)
    conductance_inverse = draw_conductance_inverse(jax.random.fold_in(splits[17], 71), 0)
    prior_voltage = noise(splits[1], (SUBS, SCENARIOS, NODES), 1.0, 6.0, ((0, 4), (2, 8)), jnp.float32)
    sources = noise(splits[2], (STEPS, SUBS, NODES), 1.0, 6.0, ((1, 4), (2, 8)), jnp.float32)
    fault_node = touch_ends(jax.random.randint(splits[3], (SCENARIOS,), 0, SUBS * NODES), jax.random.fold_in(splits[3], 1), 0, (SUBS * NODES) - 1).astype(jnp.int32)
    fault_conductance = jnp.clip(jnp.exp(jax.random.uniform(splits[4], (SCENARIOS,), jnp.float32, math.log(0.5), math.log(4.0))), 0.5, 4.0)
    terminal_node = touch_ends(jax.random.randint(splits[5], (SUBS, 3, LINE_SLOTS), 0, NODES), jax.random.fold_in(splits[5], 1), 0, NODES - 1).astype(jnp.int32)
    ownership = draw_ownership(jax.random.fold_in(splits[17], 71), 0)
    partner = draw_partner(jax.random.fold_in(splits[17], 71), 0)
    delay_steps = draw_delay_steps(jax.random.fold_in(splits[17], 71), 0)
    surge_conductance = jnp.clip(jnp.exp(math.log(1.0) - 1.609438 * jax.random.uniform(splits[9], (SUBS, LINE_SLOTS), jnp.float32) ** levels(splits[9], (SUBS, LINE_SLOTS), ((0, 4), (1, 8)), -0.2, 0.2)), 0.2, 1.0)
    pole_wave = jnp.clip(jnp.exp(math.log(0.95) - 1.5581446 * jax.random.uniform(splits[10], (SUBS, POLES, LINE_SLOTS), jnp.float32) ** levels(splits[10], (SUBS, POLES, LINE_SLOTS), ((0, 4), (2, 8)), -0.2, 0.2)), 0.2, 0.95)
    residue_wave = noise(splits[11], (SUBS, POLES, 3, 3, LINE_SLOTS), 0.15, 1.0, ((0, 4), (4, 8)), jnp.float32)
    pole_admit = jnp.clip(jnp.exp(math.log(0.95) - 1.5581446 * jax.random.uniform(splits[12], (SUBS, POLES, LINE_SLOTS), jnp.float32) ** levels(splits[12], (SUBS, POLES, LINE_SLOTS), ((0, 4), (2, 8)), -0.2, 0.2)), 0.2, 0.95)
    residue_admit = noise(splits[13], (SUBS, POLES, 3, 3, LINE_SLOTS), 0.15, 1.0, ((0, 4), (4, 8)), jnp.float32)
    wave_state = noise(splits[14], (SUBS, POLES, 3, SCENARIOS, LINE_SLOTS), 0.5, 4.0, ((0, 4), (4, 8)), jnp.float32)
    admit_state = noise(splits[15], (SUBS, POLES, 3, SCENARIOS, LINE_SLOTS), 0.5, 4.0, ((0, 4), (4, 8)), jnp.float32)
    wave_history = noise(splits[16], (SUBS, DELAY_MAX, 3, SCENARIOS, LINE_SLOTS), 1.0, 6.0, ((0, 4), (4, 8)), jnp.float32)
    return {"conductance_inverse": conductance_inverse, "prior_voltage": prior_voltage, "sources": sources, "fault_node": fault_node, "fault_conductance": fault_conductance, "terminal_node": terminal_node, "ownership": ownership, "partner": partner, "delay_steps": delay_steps, "surge_conductance": surge_conductance, "pole_wave": pole_wave, "residue_wave": residue_wave, "pole_admit": pole_admit, "residue_admit": residue_admit, "wave_state": wave_state, "admit_state": admit_state, "wave_history": wave_history}


def mix_residue(residue, vector):
    return (residue[:, :, 0, None, :] * vector[0] + residue[:, :, 1, None, :] * vector[1]
            + residue[:, :, 2, None, :] * vector[2])


def select_delayed(buffer, delay_local):
    depth_count = buffer.shape[0]
    chosen = delay_local[None, :] == jnp.arange(1, depth_count + 1, dtype=jnp.int32)[:, None]
    return jnp.sum(jnp.where(chosen[:, None, None, :], buffer, 0.0), axis=0)


def terminal_values(voltage, terminal):
    picked = jnp.take(voltage, terminal.reshape(-1), axis=1)
    return jnp.moveaxis(picked.reshape(voltage.shape[0], 3, -1), 0, 1)


def spread_ends(history, terminal, node_count):
    values = jnp.moveaxis(history, 0, 1).reshape(history.shape[1], -1)
    return jnp.zeros((history.shape[1], node_count), jnp.float32).at[:, terminal.reshape(-1)].add(values)


def split_devices(array):
    leading = array.shape[0]
    middle = array.shape[1:-1]
    shaped = array.reshape((leading,) + middle + (N_LINE, array.shape[-1] // N_LINE))
    shaped = jnp.moveaxis(shaped, -2, 1)
    return shaped.reshape((leading * N_LINE,) + middle + (shaped.shape[-1],))


def join_devices(array):
    leading = array.shape[0] // N_LINE
    middle = array.shape[1:-1]
    shaped = array.reshape((leading, N_LINE) + middle + (array.shape[-1],))
    shaped = jnp.moveaxis(shaped, 1, -2)
    return shaped.reshape((leading,) + middle + (N_LINE * array.shape[-1],))


def solve_block(operands):
    return lax.dot_general(operands[0], operands[1], (((1,), (1,)), ((), ())),
                           precision=lax.Precision.HIGHEST, preferred_element_type=jnp.float32)


def reference(conductance_inverse, prior_voltage, sources, fault_node, fault_conductance, terminal_node,
              ownership, partner, delay_steps, surge_conductance, pole_wave, residue_wave, pole_admit,
              residue_admit, wave_state, admit_state, wave_history):
    live_float = split_devices(ownership).astype(jnp.float32)
    terminal_dev = split_devices(terminal_node)
    partner_dev = split_devices(partner)
    delay_dev = split_devices(delay_steps)
    surge_dev = split_devices(surge_conductance)
    wave_decay = split_devices(pole_wave)[:, :, None, None, :]
    admit_decay = split_devices(pole_admit)[:, :, None, None, :]
    wave_res = split_devices(residue_wave)
    admit_res = split_devices(residue_admit)
    wave_now = split_devices(wave_state)
    admits = split_devices(admit_state)
    history_buffer = split_devices(wave_history)
    slot_count = live_float.shape[1]
    slot_range = jnp.arange(slot_count, dtype=jnp.int32)
    scenario_range = jnp.arange(prior_voltage.shape[1], dtype=jnp.int32)
    fault_sub = fault_node // NODES
    fault_local = fault_node % NODES
    voltage = prior_voltage
    outgoing = None
    current = None
    mixer = jax.vmap(mix_residue)
    for step_index in range(STEPS):
        if step_index > 0:
            by_slot = jnp.moveaxis(outgoing, 3, 1)
            far_waves = by_slot[partner_dev, slot_range[None, :]]
            arrived = jnp.moveaxis(far_waves, 1, 3) * live_float[:, None, None, :]
            history_buffer = jnp.concatenate([arrived[:, None], history_buffer[:, :-1]], axis=1)
        incoming = jax.vmap(select_delayed)(history_buffer, delay_dev)
        voltage_dev = jnp.repeat(voltage, N_LINE, axis=0)
        terminal_prior = jax.vmap(terminal_values)(voltage_dev, terminal_dev)
        wave_now = wave_decay * wave_now + mixer(wave_res, incoming)
        admits = admit_decay * admits + mixer(admit_res, terminal_prior)
        history = (jnp.sum(wave_now, axis=1) - jnp.sum(admits, axis=1)) * live_float[:, None, None, :]
        injection = jax.vmap(partial(spread_ends, node_count=NODES))(join_devices(history), terminal_node)
        injection = injection + sources[step_index][:, None, :]
        fault_value = voltage[fault_sub, scenario_range, fault_local]
        injection = injection.at[fault_sub, scenario_range, fault_local].add(-fault_conductance * fault_value)
        voltage = lax.map(solve_block, (injection, conductance_inverse))
        voltage_dev = jnp.repeat(voltage, N_LINE, axis=0)
        terminal_now = jax.vmap(terminal_values)(voltage_dev, terminal_dev)
        if step_index + 1 < STEPS:
            outgoing = (2.0 * surge_dev[:, None, None, :] * terminal_now - history) * live_float[:, None, None, :]
        else:
            current = (surge_dev[:, None, None, :] * terminal_now - history) * live_float[:, None, None, :]
    return voltage, join_devices(current)
```

```python
import functools

import jax
import jax.numpy as jnp
from jax import lax
from jax.experimental import pallas as pl
from jax.experimental.pallas import tpu as pltpu
from jax.sharding import PartitionSpec as P

STEPS = 3
CORES = 2
MESH = pl.DeviceIdType.MESH


def mix_residue(residue, vector):
    return (
        residue[:, :, 0, None, :] * vector[0]
        + residue[:, :, 1, None, :] * vector[1]
        + residue[:, :, 2, None, :] * vector[2]
    )


def select_delayed(buffer, delay_local):
    depth_count = buffer.shape[0]
    chosen = delay_local[None, :] == jnp.arange(1, depth_count + 1, dtype=jnp.int32)[:, None]
    return jnp.sum(jnp.where(chosen[:, None, None, :], buffer, 0.0), axis=0)


def split_two(value):
    high = value.astype(jnp.bfloat16)
    low = (value - high.astype(jnp.float32)).astype(jnp.bfloat16)
    return high, low


def dot_nt(left, right):
    return lax.dot_general(left, right, (((1,), (1,)), ((), ())), preferred_element_type=jnp.float32)


def dot_nn(left, right):
    return lax.dot_general(left, right, (((1,), (0,)), ((), ())), preferred_element_type=jnp.float32)


def positions(chips):
    line = lax.axis_index("line")
    return line, line // CORES, line % CORES


def greet(chips):
    line, z, core = positions(chips)
    barrier = pltpu.get_barrier_semaphore()
    pl.semaphore_signal(barrier, inc=1, device_id={"line": z * CORES + 1 - core}, device_id_type=MESH)
    for i in range(chips - 1):
        peer = lax.rem(z + 1 + i, chips) * CORES + core
        pl.semaphore_signal(barrier, inc=1, device_id={"line": peer}, device_id_type=MESH)
    pl.semaphore_wait(barrier, chips)


def remote(src, dst, send, recv, line_index):
    return pltpu.make_async_remote_copy(
        src_ref=src, dst_ref=dst, send_sem=send, recv_sem=recv,
        device_id={"line": line_index}, device_id_type=MESH,
    )


def gather_blocks(chips, buf, sems, consume):
    c_send, c_recv, d_send, d_recv = sems
    line, z, core = positions(chips)
    partner = z * CORES + 1 - core

    def across(i):
        peer = lax.rem(z + 1 + i, chips) * CORES + core
        return remote(buf.at[line], buf.at[line], c_send.at[i], c_recv.at[i], peer)

    def over(i, block):
        return remote(buf.at[block], buf.at[block], d_send.at[i], d_recv.at[i], partner)

    for i in range(chips - 1):
        across(i).start()

    def step(k, carry):
        i = lax.rem(k + chips - 1, chips)
        source = lax.rem(z + 2 * chips - 1 - i, chips)
        block = source * CORES + core

        @pl.when(k > 0)
        def _():
            remote(buf.at[block], buf.at[block], c_send.at[i], c_recv.at[i], partner).wait_recv()

        over(i, block).start()
        consume(block)
        other = source * CORES + 1 - core
        remote(buf.at[other], buf.at[other], d_send.at[i], d_recv.at[i], partner).wait_recv()
        consume(other)
        return carry

    lax.fori_loop(0, chips, step, 0)
    for i in range(chips - 1):
        across(i).wait_send()
    for i in range(chips):
        source = lax.rem(z + 2 * chips - 1 - i, chips)
        over(i, source * CORES + core).wait_send()


def one_hot(term_ref, phase, block, width):
    slots = term_ref.shape[1]
    rows = lax.broadcasted_iota(jnp.int32, (width, slots), 0) + block * width
    return (rows == term_ref[phase : phase + 1, :]).astype(jnp.float32).astype(jnp.bfloat16)


def pick_terminals(chips, buf, sems, term_ref, ends_ref):
    phases, count, _ = ends_ref.shape
    width = buf.shape[2]
    ends_ref[...] = jnp.zeros_like(ends_ref)

    def consume(block):
        both = jnp.concatenate(split_two(buf[block]), axis=0)
        for p in range(phases):
            got = dot_nn(both, one_hot(term_ref, p, block, width))
            ends_ref[p] += got[:count] + got[count:]

    gather_blocks(chips, buf, sems, consume)


def prior_kernel(chips, prior_ref, term_ref, ends_ref, vfull, *sems):
    line, z, core = positions(chips)
    greet(chips)
    vfull[line] = prior_ref[...]
    pick_terminals(chips, vfull, sems, term_ref, ends_ref)


def step_kernel(
    chips, h_ref, term_ref, add_ref, inv_hbm, volt_ref, ends_ref,
    part, r1, summed, r2, ifull, vfull, inv, inv_sem,
    a_send, a_recv, b_send, b_recv, *sems,
):
    line, z, core = positions(chips)
    partner = z * CORES + 1 - core
    phases = h_ref.shape[0]
    count, width = add_ref.shape
    load = pltpu.make_async_copy(inv_hbm, inv, inv_sem)
    load.start()
    greet(chips)

    def scatter_block(block):
        total = jnp.zeros((count, width), jnp.float32)
        for p in range(phases):
            both = jnp.concatenate(split_two(h_ref[p]), axis=0)
            got = dot_nt(both, one_hot(term_ref, p, block, width))
            total = total + (got[:count] + got[count:])
        return total

    def swap(i):
        return remote(part.at[i], r1.at[i], a_send.at[i], a_recv.at[i], partner)

    def pass_on(i):
        peer = lax.rem(z + 1 + i, chips) * CORES + core
        return remote(summed.at[i], r2.at[i], b_send.at[i], b_recv.at[i], peer)

    def scatter_step(i, carry):
        target = lax.rem(z + 1 + i, chips)
        part[i] = scatter_block(target * CORES + 1 - core)
        swap(i).start()
        own = scatter_block(target * CORES + core)
        swap(i).wait_recv()
        summed[i] = own + r1[i]

        @pl.when(i < chips - 1)
        def _():
            pass_on(i).start()

        return carry

    lax.fori_loop(0, chips, scatter_step, 0)
    total = summed[chips - 1] + add_ref[...]
    for i in range(chips - 1):
        pass_on(i).wait_recv()
        total = total + r2[i]
    ifull[line] = total
    load.wait()
    volt_ref[...] = jnp.zeros_like(volt_ref)

    def solve(block):
        both = jnp.concatenate(split_two(ifull[block]), axis=0)
        start = pl.multiple_of(block * width, width)
        high, low = split_two(inv[:, pl.ds(start, width)])
        got = dot_nt(both, high)
        volt_ref[...] += got[:count] + (got[count:] + dot_nt(both[:count], low))

    gather_blocks(chips, ifull, sems[:4], solve)
    vfull[line] = volt_ref[...]
    pick_terminals(chips, vfull, sems[4:], term_ref, ends_ref)
    for i in range(chips):
        swap(i).wait_send()
    for i in range(chips - 1):
        pass_on(i).wait_send()


def gather_sems(chips):
    return [
        pltpu.SemaphoreType.DMA((chips,)),
        pltpu.SemaphoreType.DMA((chips,)),
        pltpu.SemaphoreType.DMA((chips,)),
        pltpu.SemaphoreType.DMA((chips,)),
    ]


def vmem():
    return pl.BlockSpec(memory_space=pltpu.VMEM)


def prior_ends(prior, terminal, lines):
    chips = lines // CORES
    count, width = prior.shape
    return pl.pallas_call(
        functools.partial(prior_kernel, chips),
        out_shape=jax.ShapeDtypeStruct((terminal.shape[0], count, terminal.shape[1]), jnp.float32),
        in_specs=[vmem(), vmem()],
        out_specs=vmem(),
        scratch_shapes=[pltpu.VMEM((lines, count, width), jnp.float32)] + gather_sems(chips),
        compiler_params=pltpu.CompilerParams(collective_id=1, has_side_effects=True),
        name="prior_ends",
    )(prior, terminal)


def network_step(h, terminal, extra, inverse, lines):
    chips = lines // CORES
    count, width = extra.shape
    block = lambda n: pltpu.VMEM((n, count, width), jnp.float32)
    return pl.pallas_call(
        functools.partial(step_kernel, chips),
        out_shape=(
            jax.ShapeDtypeStruct((count, width), jnp.float32),
            jax.ShapeDtypeStruct(h.shape, jnp.float32),
        ),
        in_specs=[vmem(), vmem(), vmem(), pl.BlockSpec(memory_space=pltpu.HBM)],
        out_specs=(vmem(), vmem()),
        scratch_shapes=[
            block(chips), block(chips), block(chips), block(chips), block(lines), block(lines),
            pltpu.VMEM(inverse.shape, jnp.float32),
            pltpu.SemaphoreType.DMA(()),
        ] + gather_sems(chips) + gather_sems(chips) + gather_sems(chips),
        compiler_params=pltpu.CompilerParams(
            collective_id=0, has_side_effects=True, vmem_limit_bytes=40 * 2**20
        ),
        name="network_step",
    )(h, terminal, extra, inverse)


def on_device(
    conductance_inverse,
    prior_voltage,
    sources,
    fault_node,
    fault_conductance,
    terminal_node,
    ownership,
    partner,
    delay_steps,
    surge_conductance,
    pole_wave,
    residue_wave,
    pole_admit,
    residue_admit,
    wave_state,
    admit_state,
    wave_history,
):
    inverse_block = conductance_inverse[0]
    row_count = inverse_block.shape[0]
    node_count = inverse_block.shape[1]
    line_index = lax.axis_index("line")
    net_index = lax.axis_index("net")
    line_count = lax.axis_size("line")
    devices = lax.axis_size("net") * line_count
    slot_count = ownership.shape[1]
    capacity = (slot_count + devices - 2) // (devices - 1)
    is_live = ownership[0] > 0
    live_float = is_live.astype(jnp.float32)
    terminal = terminal_node[0]
    delay_local = delay_steps[0]
    surge_local = surge_conductance[0]
    partners = partner[0]
    slot_range = jnp.arange(slot_count, dtype=jnp.int32)
    earlier = (
        (partners[:, None] == partners[None, :])
        & is_live[:, None]
        & (slot_range[:, None] < slot_range[None, :])
    )
    slot_rank = jnp.sum(earlier.astype(jnp.int32), axis=0)
    position = jnp.where(is_live, partners * capacity + slot_rank, devices * capacity)
    place = jnp.arange(devices * capacity, dtype=jnp.int32)
    packer = (place[:, None] == position[None, :]).astype(jnp.float32)
    fault_local = fault_node - (net_index * node_count + line_index * row_count)
    fault_hit = fault_local[:, None] == jnp.arange(row_count, dtype=jnp.int32)[None, :]
    fault_weight = jnp.where(fault_hit, fault_conductance[:, None], 0.0)
    wave_decay = pole_wave[0][:, None, None, :]
    admit_decay = pole_admit[0][:, None, None, :]
    wave_res = residue_wave[0]
    admit_res = residue_admit[0]
    voltage_rows = prior_voltage[0]
    wave_now = wave_state[0]
    admits = admit_state[0]
    history_buffer = wave_history[0]
    ends = prior_ends(voltage_rows, terminal, line_count)
    outgoing = None
    current = None
    for step_index in range(STEPS):
        if step_index == 0:
            wave_now = wave_decay * wave_now + mix_residue(
                wave_res, select_delayed(history_buffer, delay_local)
            )
            admits = admit_decay * admits + mix_residue(admit_res, ends)
        else:
            rows = outgoing.reshape(-1, slot_count)
            buffer = lax.dot_general(
                packer, rows, (((1,), (1,)), ((), ())), precision=lax.Precision.HIGHEST
            )
            arrived = lax.all_to_all(
                buffer, ("net", "line"), split_axis=0, concat_axis=0, tiled=True
            )
            admits = admit_decay * admits + mix_residue(admit_res, ends)
            arrived = lax.dot_general(
                arrived, packer, (((0,), (0,)), ((), ())), precision=lax.Precision.HIGHEST
            ).reshape(outgoing.shape)
            history_buffer = jnp.concatenate([arrived[None], history_buffer[:-1]], axis=0)
            wave_now = wave_decay * wave_now + mix_residue(
                wave_res, select_delayed(history_buffer, delay_local)
            )
        history = (jnp.sum(wave_now, axis=0) - jnp.sum(admits, axis=0)) * live_float
        extra = sources[step_index, 0][None, :] - fault_weight * voltage_rows
        voltage_rows, ends = network_step(history, terminal, extra, inverse_block, line_count)
        if step_index + 1 < STEPS:
            outgoing = (2.0 * surge_local * ends - history) * live_float
        else:
            current = (surge_local * ends - history) * live_float
    return (voltage_rows[None], current[None])


def solution(mesh):
    return jax.shard_map(
        on_device,
        mesh=mesh,
        in_specs=(
            P("net", "line", None),
            P("net", None, "line"),
            P(None, "net", "line"),
            P(),
            P(),
            P("net", None, "line"),
            P("net", "line"),
            P("net", "line"),
            P("net", "line"),
            P("net", "line"),
            P("net", None, "line"),
            P("net", None, None, None, "line"),
            P("net", None, "line"),
            P("net", None, None, None, "line"),
            P("net", None, None, None, "line"),
            P("net", None, None, None, "line"),
            P("net", None, None, None, "line"),
        ),
        out_specs=(P("net", None, "line"), P("net", None, None, "line")),
        check_vma=False,
    )
```
